256 devices in a mesh: wide: 64 (over z_lo, x, y, core), narrow: 4 (over z_hi).
Axes of the slice: x: 4, y: 4, z: 8 (z_hi: 4, z_lo: 2; z = z_hi * 2 + z_lo), core: 2. Of those that a mesh axis runs over, the one named last changes fastest.
Arguments:
- queries: bfloat16 [131072, 768], P(('wide', 'narrow')), may hold values from -150 to 150
- documents: bfloat16 [8192, 768], P(('wide', 'narrow')), may hold values from -5 to 5
- positives: int32 [131072], P(('wide', 'narrow')), may hold values from 0 to 8191
Outputs:
- losses: float32 [131072], P(('wide', 'narrow'))
- query_grad: bfloat16 [131072, 768], P(('wide', 'narrow'))
The draws below stay inside these ranges and needn't reach their ends.
All inputs are finite; a program needn't handle non-finite values. Where the reference program divides by a largest or mean magnitude, that divisor is 1e-20 or more.
Results may differ from the reference program's by a relative error of at most 0.005.
Values may be sent and summed in bfloat16 or wider, within the bound.
A program may use at most 64 MiB of HBM per device.

```python
import jax
import jax.numpy as jnp
from jax import lax

E = 768
QUERIES = 131072
DOCS = 8192


def base_documents(key):
    values = jax.random.normal(jax.random.fold_in(key, 11), (DOCS, E), jnp.float32)
    return jnp.clip(values, -5.0, 5.0)


def draw_documents(key, part):
    return base_documents(key).astype(jnp.bfloat16)


def draw_queries(key, part):
    values = jnp.clip(jax.random.normal(jax.random.fold_in(key, 12), (QUERIES, E), jnp.float32), -5.0, 5.0)
    return values.astype(jnp.bfloat16)


def set_ends(entries, stream_key, least, largest):
    longest = entries.shape.index(max(entries.shape))
    spots = []
    for shift in (0, 1):
        where = [jax.random.randint(jax.random.fold_in(stream_key, axis), (), 0, length) for axis, length in enumerate(entries.shape)]
        where[longest] = (where[longest] + shift) % entries.shape[longest]
        spots.append(tuple(where))
    return entries.at[spots[0]].set(least).at[spots[1]].set(largest)


def setup_inputs(seed: int = 0) -> dict:
    streams_of = jax.random.split(jax.random.key(seed), 4)
    return {
        "queries": draw_queries(jax.random.fold_in(streams_of[3], 71), 0),
        "documents": draw_documents(jax.random.fold_in(streams_of[3], 71), 0),
        "positives": set_ends(jax.random.randint(streams_of[2], (QUERIES,), 0, DOCS), jax.random.fold_in(streams_of[2], 1), 0, DOCS - 1).astype(jnp.int32),
    }


def reference(queries, documents, positives):
    temper = E ** -0.5
    doc_values = documents.astype(jnp.float32)
    scales = jnp.max(jnp.abs(doc_values), axis=1) + 1e-6
    codes = (doc_values / scales[:, None]).astype(jnp.bfloat16)
    qblock = min(512, QUERIES)
    count = QUERIES // qblock
    query_blocks = queries.reshape(count, qblock, E)
    pos_blocks = positives.reshape(count, qblock)
    column_ids = jnp.arange(DOCS, dtype=jnp.int32)

    def one_block(pair):
        rows, picks = pair
        raw = jnp.dot(rows, codes.T, preferred_element_type=jnp.float32)
        scores = raw * scales[None, :] * temper
        top = jnp.max(scores, axis=1)
        lse = top + jnp.log(jnp.sum(jnp.exp(scores - top[:, None]), axis=1))
        hit = column_ids[None, :] == picks[:, None]
        chosen = jnp.sum(jnp.where(hit, scores, 0.0), axis=1)
        probs = jnp.exp(scores - lse[:, None])
        weights = ((probs - hit.astype(jnp.float32)) * scales[None, :]).astype(jnp.bfloat16)
        grad = jnp.dot(weights, codes, preferred_element_type=jnp.float32) * temper
        return lse - chosen, grad.astype(jnp.bfloat16)

    losses, grads = lax.map(one_block, (query_blocks, pos_blocks))
    return losses.reshape(QUERIES), grads.reshape(QUERIES, E)
```

```python
import jax
import jax.numpy as jnp
from jax import lax
from jax.experimental import pallas as pl
from jax.experimental.pallas import tpu as pltpu
from jax.sharding import PartitionSpec as P

LOG2E = 1.4426950408889634
MESH = pl.DeviceIdType.MESH
NX, NY, NZ = 4, 4, 8
RB = 32
SLOTS = 8
Y_COLS = (0, 256)
X_COLS = (256, 256)
XW_COLS = (256, 512)
W_COLS = (512, 256)
ZB_COLS = (0, 512)
W_OFF = (0, 1, 3, 2)
ROWS = 256


def kernel(
    n_copies,
    q_ref,
    d_ref,
    p_ref,
    loss_ref,
    grad_ref,
    buf,
    sbuf,
    pos,
    run_max,
    run_sum,
    chosen,
    acc,
    picked,
    s_a,
    s_b,
    send_sem,
    recv_sem,
):
    wide = lax.axis_index("wide")
    narrow = lax.axis_index("narrow")
    core = lax.rem(wide, 2)
    y = lax.rem(wide // 2, NY)
    x = lax.rem(wide // 8, NX)
    z = narrow * 2 + wide // 32
    width = q_ref.shape[1]
    temper = width**-0.5

    def xm(d):
        return lax.rem(x + d + NX, NX)

    def ym(d):
        return lax.rem(y + d + NY, NY)

    def zm(d):
        return lax.rem(z + d + NZ, NZ)

    def dev(xx, yy, zz, cc):
        return ((lax.rem(zz, 2) * NX + xx) * NY + yy) * 2 + cc, zz // 2

    at_x = lambda d: dev(xm(d), y, z, core)
    at_y = lambda d: dev(x, ym(d), z, core)
    at_z = lambda d: dev(x, y, zm(d), core)
    sibling = dev(x, y, z, 1 - core)

    docs = d_ref[...].astype(jnp.float32)
    scale = jnp.max(jnp.abs(docs), axis=1, keepdims=True) + 1e-06
    mine = (z * 2 + core) * NX + x
    my_rows = pl.ds(pl.multiple_of(y * RB, RB), RB)
    buf[mine, my_rows, :] = (docs / scale).astype(jnp.bfloat16)
    lane = lax.broadcasted_iota(jnp.int32, (RB, 128), 1)
    row = lax.broadcasted_iota(jnp.int32, (RB, 128), 0)
    sbuf[z, core, x * NY + y] = jnp.sum(
        jnp.where(lane == row + y * RB, scale, 0.0), axis=0, keepdims=True
    )

    barrier = pltpu.get_barrier_semaphore()
    peers = (
        [sibling]
        + [at_x(d) for d in (1, 2, 3)]
        + [at_y(d) for d in (1, 2, 3)]
        + [at_z(d) for d in range(1, NZ)]
    )
    for peer in peers:
        pl.semaphore_signal(barrier, inc=1, device_id=peer, device_id_type=MESH)
    pl.semaphore_wait(barrier, len(peers))

    index = {}
    draining = []

    def copy_of(key, ref, peer):
        i = index.setdefault(key, len(index))
        return pltpu.make_async_remote_copy(
            src_ref=ref,
            dst_ref=ref,
            send_sem=send_sem.at[i],
            recv_sem=recv_sem.at[i],
            device_id=peer,
            device_id_type=MESH,
        )

    def send(key, ref, peer):
        copy = copy_of(key, ref, peer)
        if draining:
            copy.wait_send()
        else:
            copy.start()

    def arrive(key, ref):
        if not draining:
            copy_of(key, ref, sibling).wait_recv()

    def cell(plane, xx):
        return (plane * 2 + core) * NX + xx

    def block(plane, xx, yy, cols, first=0, rows=RB):
        start = pl.multiple_of(yy * RB + first, 16)
        return buf.at[cell(plane, xx), pl.ds(start, rows), pl.ds(*cols)]

    def y_group(plane, xx, cols, first=0, rows=NY * RB):
        return buf.at[cell(plane, xx), pl.ds(first, rows), pl.ds(*cols)]

    def x_group(plane, yy, cols, first=0, many=NX):
        start = pl.multiple_of(yy * RB, RB)
        return buf.at[
            pl.ds(cell(plane, 0) + first, many), pl.ds(start, RB), pl.ds(*cols)
        ]

    def dz(s):
        return 0 if s == 0 else (-((s + 1) // 2) if s % 2 else s // 2)

    def plane_at(s):
        return zm(dz(s))

    def x_cols(s):
        return XW_COLS if s == 0 else X_COLS

    def stage_a(s):
        p = plane_at(s)
        for d in (1, -1):
            send(("Xy", s, d), block(p, x, y, x_cols(s)), at_y(d))
            send(("Yx", s, d), block(p, x, y, Y_COLS), at_x(d))

    def stage_b(s):
        p = plane_at(s)
        for d in (1, -1):
            half = 0 if d == 1 else RB // 2
            arrive(("Xy", s, d), block(p, x, ym(-d), x_cols(s)))
            send(
                ("XyF", s, d),
                block(p, x, ym(-d), x_cols(s), half, RB // 2),
                at_y(d),
            )
            arrive(("Yx", s, d), block(p, xm(-d), y, Y_COLS))
            send(
                ("YxF", s, d), block(p, xm(-d), y, Y_COLS, half, RB // 2), at_x(d)
            )

    def stage_c(s):
        p = plane_at(s)
        for d in (1, -1):
            half = 0 if d == 1 else RB // 2
            arrive(("XyF", s, d), block(p, x, ym(2), x_cols(s), half, RB // 2))
            arrive(("YxF", s, d), block(p, xm(2), y, Y_COLS, half, RB // 2))
        for d in (1, -1):
            send(("Xx", s, d), y_group(p, x, x_cols(s)), at_x(d))
            send(("Yy", s, d), x_group(p, y, Y_COLS), at_y(d))

    def stage_d(s):
        p = plane_at(s)
        for d in (1, -1):
            half = 0 if d == 1 else 1
            arrive(("Xx", s, d), y_group(p, xm(-d), x_cols(s)))
            send(
                ("XxF", s, d),
                y_group(p, xm(-d), x_cols(s), half * 2 * RB, 2 * RB),
                at_x(d),
            )
            arrive(("Yy", s, d), x_group(p, ym(-d), Y_COLS))
            send(
                ("YyF", s, d), x_group(p, ym(-d), Y_COLS, half * 2, 2), at_y(d)
            )

    def stage_e(s):
        p = plane_at(s)
        for d in (1, -1):
            half = 0 if d == 1 else 1
            arrive(
                ("XxF", s, d), y_group(p, xm(2), x_cols(s), half * 2 * RB, 2 * RB)
            )
            arrive(("YyF", s, d), x_group(p, ym(2), Y_COLS, half * 2, 2))

    def w_piece(h, g, d):
        return y_group(zm(-d * h), xm(W_OFF[g]), W_COLS)

    def w_final(g, d):
        return (g < 2) == (d == 1)

    def w_send(h, g, d):
        if h > 4 or (h == 4 and not w_final(g, d)):
            return
        send(("W", h, g, d), w_piece(h - 1, g, d), at_z(d))

    def w_arrive(h, g, d):
        if h > 4 or (h == 4 and not w_final(g, d)):
            return
        arrive(("W", h, g, d), w_piece(h, g, d))

    def zb_cols(h, d):
        return ZB_COLS if h < 4 else (Y_COLS if d == 1 else X_COLS)

    def z_send(h, d):
        send(
            ("Z", h, d), block(zm(-d * (h - 1)), x, y, zb_cols(h, d)), at_z(d)
        )

    def z_arrive(h, d):
        arrive(("Z", h, d), block(zm(-d * h), x, y, zb_cols(h, d)))

    def plane_ref(s, cc):
        return buf.at[pl.ds((plane_at(s) * 2 + cc) * NX, NX)]

    def comm(t):
        both = (1, -1)
        if t == 0:
            stage_a(0)
            for d in both:
                z_send(1, d)
            for d in (1, 2, 3):
                send(("Sy", d), sbuf.at[z, core, x * NY + y], at_y(d))
            return
        if t == 1:
            for d in both:
                z_arrive(1, d)
                z_send(2, d)
            stage_b(0)
            stage_a(1)
            for d in (1, 2, 3):
                arrive(("Sy", d), sbuf.at[z, core, x * NY + ym(-d)])
            for d in (1, 2, 3):
                send(("Sx", d), sbuf.at[z, core, pl.ds(x * NY, NY)], at_x(d))
            return
        if 0 <= t - 4 < SLOTS:
            stage_e(t - 4)
        if t == 2:
            for d in both:
                z_arrive(2, d)
                z_send(3, d)
        if t == 3:
            for d in both:
                z_arrive(3, d)
                z_send(4, d)
        if t == 4:
            for d in both:
                z_arrive(4, d)
            for d in both:
                w_send(1, 3, d)
        if 4 <= t <= 10:
            for n in (2 * (t - 4), 2 * (t - 4) + 1):
                h, g = n // 4 + 1, n % 4
                if t < 10:
                    for d in both:
                        w_arrive(h, g, d)
                        w_send(h + 1, g, d)
            if t == 10:
                for g in range(4):
                    for d in both:
                        w_arrive(4, g, d)
        if 0 <= t - 4 < SLOTS:
            send(("D", t - 4), plane_ref(t - 4, core), sibling)
        if 0 <= t - 3 < SLOTS:
            stage_d(t - 3)
        if t == 3:
            for g in (1, 2):
                for d in both:
                    w_send(1, g, d)
        if 0 <= t - 2 < SLOTS:
            stage_c(t - 2)
        if t == 2:
            for d in both:
                w_send(1, 0, d)
        if 0 <= t - 1 < SLOTS:
            stage_b(t - 1)
        if t < SLOTS:
            stage_a(t)
        if t == 2:
            for d in (1, 2, 3):
                arrive(("Sx", d), sbuf.at[z, core, pl.ds(xm(-d) * NY, NY)])
            for d in range(1, NZ):
                send(("Sz", d), sbuf.at[z, core], at_z(d))
        if t == 3:
            for d in range(1, NZ):
                arrive(("Sz", d), sbuf.at[zm(-d), core])
            send(("Sd",), sbuf.at[:, core], sibling)
        if t == 4:
            arrive(("Sd",), sbuf.at[:, 1 - core])
        if 0 <= t - 5 < SLOTS:
            arrive(("D", t - 5), plane_ref(t - 5, 1 - core))

    def codes_of(plane, cc):
        return buf[pl.ds((plane * 2 + cc) * NX, NX)].reshape(NX * NY * RB, width)

    def scores(plane, cc, out):
        codes = codes_of(plane, cc)
        for first in range(0, q_ref.shape[0], ROWS):
            rows = pl.ds(first, ROWS)
            out[rows, :] = lax.dot_general(
                q_ref[rows, :],
                codes,
                (((1,), (1,)), ((), ())),
                preferred_element_type=jnp.float32,
            )

    def fold(values, op):
        out = values[:, 0:128]
        for j in range(1, values.shape[1] // 128):
            out = op(out, values[:, j * 128 : (j + 1) * 128])
        return out

    def consume(plane, cc, raw):
        codes = codes_of(plane, cc)
        count = codes.shape[0]
        by_y = sbuf[plane, cc]
        scales = jnp.concatenate(
            [jnp.sum(by_y[i * NY : (i + 1) * NY], axis=0) for i in range(NX)], axis=1
        )
        factor = scales * (temper * LOG2E)
        start = (plane * 2 + cc) * count
        for first in range(0, q_ref.shape[0], ROWS):
            rows = pl.ds(first, ROWS)
            s = raw[rows, :] * factor
            old = run_max[rows, :]
            new = jnp.maximum(
                old, jnp.max(fold(s, jnp.maximum), axis=1, keepdims=True)
            )
            run_max[rows, :] = new
            alpha = jnp.exp2(old - new)
            p = jnp.exp2(s - new[:, 0:1])
            hit = lax.broadcasted_iota(jnp.int32, s.shape, 1) == (
                pos[rows, 0:1] - start
            )
            run_sum[rows, :] = run_sum[rows, :] * alpha + fold(p, jnp.add)
            chosen[rows, :] += fold(jnp.where(hit, s, 0.0), jnp.add)
            weights = jnp.where(hit, 0.0, p * scales).astype(jnp.bfloat16)
            onehot = jnp.where(hit, scales, 0.0).astype(jnp.bfloat16)
            spread = jnp.concatenate([alpha] * (width // 128), axis=1)
            acc[rows, :] = acc[rows, :] * spread + jnp.dot(
                weights, codes, preferred_element_type=jnp.float32
            )
            picked[rows, :] += jnp.dot(
                onehot, codes, preferred_element_type=jnp.float32
            )

    def diagonal():
        shape = (128, 128)
        return lax.broadcasted_iota(jnp.int32, shape, 0) == lax.broadcasted_iota(
            jnp.int32, shape, 1
        )

    def prepare():
        j = p_ref[...]
        device = j // RB
        w = device // 4
        jz = lax.rem(device, 4) * 2 + w // 32
        flat = (
            (jz * 2 + lax.rem(w, 2)) * NX + lax.rem(w // 8, NX)
        ) * (NY * RB) + lax.rem(w // 2, NY) * RB + lax.rem(j, RB)
        flat = flat.astype(jnp.float32)
        for i in range(flat.shape[0]):
            column = jnp.sum(
                jnp.where(diagonal(), flat[i : i + 1, :], 0.0), axis=1, keepdims=True
            )
            pos[pl.ds(i * 128, 128), :] = jnp.broadcast_to(
                column, (128, 128)
            ).astype(jnp.int32)
        run_max[...] = jnp.full_like(run_max, -1e30)
        run_sum[...] = jnp.zeros_like(run_sum)
        chosen[...] = jnp.zeros_like(chosen)
        acc[...] = jnp.zeros_like(acc)
        picked[...] = jnp.zeros_like(picked)

    comm(0)
    prepare()
    for t in range(1, 5):
        comm(t)
    scores(plane_at(0), core, s_a)

    last = SLOTS + 4

    def tick(t, carry):
        for k in range(5, last + 1):

            @pl.when(t == k)
            def _():
                comm(k)

        def plane_dyn(s):
            k = (s + 1) // 2
            return lax.rem(z + k * (1 - 2 * lax.rem(s, 2)) + NZ, NZ)

        here = plane_dyn(t - 5)
        after = plane_dyn(jnp.minimum(t - 4, SLOTS - 1))
        scores(here, 1 - core, s_b)
        consume(here, core, s_a)
        scores(after, core, s_a)
        consume(here, 1 - core, s_b)
        return carry

    lax.fori_loop(5, last + 1, tick, 0)
    draining.append(True)
    for t in range(last + 1):
        comm(t)
    assert len(index) == n_copies, len(index)

    total = jnp.sum(run_sum[...], axis=1, keepdims=True)
    lse = run_max[:, 0:1] + jnp.log2(total)
    score = jnp.sum(chosen[...], axis=1, keepdims=True)
    losses = (lse - score) * (1.0 / LOG2E)
    for i in range(loss_ref.shape[0]):
        loss_ref[pl.ds(i, 1), :] = jnp.sum(
            jnp.where(diagonal(), losses[i * 128 : (i + 1) * 128], 0.0),
            axis=0,
            keepdims=True,
        )
    extra = jnp.exp2(score - lse) - 1.0
    inverse = 1.0 / total
    grad_ref[...] = (temper * (acc[...] * inverse + extra * picked[...])).astype(
        grad_ref.dtype
    )


N_COPIES = 186


def shards(queries, documents, positives):
    count, width = queries.shape
    vmem = pl.BlockSpec(memory_space=pltpu.VMEM)
    f32 = jnp.float32
    losses, grad = pl.pallas_call(
        lambda *refs: kernel(N_COPIES, *refs),
        out_shape=(
            jax.ShapeDtypeStruct((count // 128, 128), f32),
            jax.ShapeDtypeStruct((count, width), queries.dtype),
        ),
        in_specs=[vmem] * 3,
        out_specs=(vmem, vmem),
        scratch_shapes=[
            pltpu.VMEM((NZ * 2 * NX, NY * RB, width), jnp.bfloat16),
            pltpu.VMEM((NZ, 2, NX * NY, 1, 128), f32),
            pltpu.VMEM((count, 128), jnp.int32),
            pltpu.VMEM((count, 128), f32),
            pltpu.VMEM((count, 128), f32),
            pltpu.VMEM((count, 128), f32),
            pltpu.VMEM((count, width), f32),
            pltpu.VMEM((count, width), f32),
            pltpu.VMEM((count, 512), f32),
            pltpu.VMEM((count, 512), f32),
            pltpu.SemaphoreType.DMA((N_COPIES,)),
            pltpu.SemaphoreType.DMA((N_COPIES,)),
        ],
        compiler_params=pltpu.CompilerParams(
            collective_id=0, has_side_effects=True, vmem_limit_bytes=56 * 2**20
        ),
        name="gather_softmax",
    )(queries, documents, positives.reshape(count // 128, 128))
    return losses.reshape(count), grad


def solution(mesh):
    placed = (P(("wide", "narrow"), None), P(("wide", "narrow"), None), P(("wide", "narrow")))
    return jax.shard_map(
        shards,
        mesh=mesh,
        in_specs=placed,
        out_specs=(P(("wide", "narrow")), P(("wide", "narrow"), None)),
        check_vma=False,
    )
```

```python
import jax
import jax.numpy as jnp
import numpy as np
from jax import lax
from jax.experimental import pallas as pl
from jax.experimental.pallas import tpu as pltpu
from jax.sharding import PartitionSpec as P

LOG2E = 1.4426950408889634
MESH = pl.DeviceIdType.MESH
NX, NY, NZ = 4, 4, 8
RB = 32
SLOTS = 8
Y_COLS = (0, 256)
X_COLS = (256, 256)
Y0_COLS = (0, 384)
X0_COLS = (384, 384)
W_COLS = (512, 256)
ZB_COLS = (0, 512)
W_OFF = (0, 1, 3, 2)
ROWS = 256
PLAN = (
    (("A", 0), ("Z", 1),),
    (("Z", 2), ("A", 1), ("A", 2), ("C", 0), ("W", 1, 0), ("B", 1), ("Z", 3), ("A", 3), ("B", 2), ("A", 4), ("W", 2, 0), ("D", 0), ("Z", 4), ("W", 1, 1), ("W", 1, 2), ("C", 1), ("A", 5), ("A", 6), ("B", 3), ("C", 2), ("B", 4), ("W", 3, 0), ("E", 0), ("W", 1, 3), ("A", 7),),
    (("D", 1), ("W", 2, 1),),
    (("W", 2, 2), ("C", 3), ("B", 5), ("B", 6), ("D", 2), ("C", 4), ("B", 7), ("W", 4, 0), ("E", 1), ("W", 2, 3),),
    (("D", 3), ("W", 3, 1), ("C", 5),),
    (("E", 2), ("W", 3, 2),),
    (("E", 3), ("D", 4), ("C", 6), ("W", 5, 0),),
    (("W", 3, 3), ("D", 5), ("C", 7),),
    (("E", 4), ("W", 4, 1),),
    (("D", 6), ("E", 5), ("W", 4, 2),),
    (("W", 4, 3), ("D", 7),),
    (("E", 6), ("W", 5, 1),),
    (("E", 7), ("W", 5, 2),),
    (("W", 5, 3),),
    (),
    (),
    (),
    (),
)


def kernel(
    q_ref,
    d_ref,
    p_ref,
    loss_ref,
    grad_ref,
    buf,
    sbuf,
    pos,
    run_max,
    run_sum,
    chosen,
    acc,
    picked,
    s_a,
    s_b,
    send_sem,
    recv_sem,
):
    wide = lax.axis_index("wide")
    narrow = lax.axis_index("narrow")
    core = lax.rem(wide, 2)
    y = lax.rem(wide // 2, NY)
    x = lax.rem(wide // 8, NX)
    z = narrow * 2 + wide // 32
    width = q_ref.shape[1]
    temper = width**-0.5

    def xm(d):
        return lax.rem(x + d + NX, NX)

    def ym(d):
        return lax.rem(y + d + NY, NY)

    def zm(d):
        return lax.rem(z + d + NZ, NZ)

    def dev(xx, yy, zz, cc):
        return ((lax.rem(zz, 2) * NX + xx) * NY + yy) * 2 + cc, zz // 2

    at_x = lambda d: dev(xm(d), y, z, core)
    at_y = lambda d: dev(x, ym(d), z, core)
    at_z = lambda d: dev(x, y, zm(d), core)
    sibling = dev(x, y, z, 1 - core)

    docs = d_ref[...].astype(jnp.float32)
    scale = jnp.max(jnp.abs(docs), axis=1, keepdims=True) + 1e-06
    mine = (z * 2 + core) * NX + x
    my_rows = pl.ds(pl.multiple_of(y * RB, RB), RB)
    buf[mine, my_rows, :] = (docs / scale).astype(jnp.bfloat16)
    lane = lax.broadcasted_iota(jnp.int32, (RB, 128), 1)
    row = lax.broadcasted_iota(jnp.int32, (RB, 128), 0)
    sbuf[z, core, x * NY + y] = jnp.sum(
        jnp.where(lane == row + y * RB, scale, 0.0), axis=0, keepdims=True
    )

    barrier = pltpu.get_barrier_semaphore()
    peers = (
        [sibling]
        + [at_x(d) for d in (1, 2, 3)]
        + [at_y(d) for d in (1, 2, 3)]
        + [at_z(d) for d in range(1, NZ)]
    )
    for peer in peers:
        pl.semaphore_signal(barrier, inc=1, device_id=peer, device_id_type=MESH)
    pl.semaphore_wait(barrier, len(peers))

    recv_index = {}
    send_index = {}
    totals = {}
    waited = set()

    def send(group, lane, ref, peer):
        pltpu.make_async_remote_copy(
            src_ref=ref,
            dst_ref=ref,
            send_sem=send_sem.at[send_index.setdefault(lane, len(send_index))],
            recv_sem=recv_sem.at[recv_index.setdefault(group, len(recv_index))],
            device_id=peer,
            device_id_type=MESH,
        ).start()
        totals[lane] = totals.get(lane, 0) + int(np.prod(ref.shape)) * ref.dtype.itemsize

    def dummy(tiles):
        for rows, cols in ((128, 768), (128, 256), (64, 256), (16, 256)):
            unit = rows * cols // 4096
            if tiles % unit == 0 and tiles // unit <= buf.shape[0]:
                return buf.at[pl.ds(0, tiles // unit), pl.ds(0, rows), pl.ds(0, cols)]
        raise ValueError(tiles)

    def semaphore_copy(ref, send_at, recv_at):
        return pltpu.make_async_remote_copy(
            src_ref=ref,
            dst_ref=ref,
            send_sem=send_sem.at[send_at],
            recv_sem=recv_sem.at[recv_at],
            device_id=sibling,
            device_id_type=MESH,
        )

    def scale_ref(rows):
        if rows % 16:
            return sbuf.at[0, 0, pl.ds(0, rows)]
        return sbuf.at[pl.ds(0, rows // 16), 0]

    def arrived(group):
        k = group[0]
        if k == "sc":
            return scale_ref((0, 3, 12, 112, 128)[group[1]])
        s = group[1]
        if k == "A":
            size = 144 if s == 0 else 64
        elif k == "B":
            size = 32
        elif k == "C":
            size = 384 if s == 0 else 256
        elif k == "D":
            size = 192 if s == 0 else 128
        elif k == "Z":
            size = 64 if s < 4 else 32
        elif k == "W":
            size = 128 if s < 4 else 64
        else:
            size = 768
        return dummy(size // 8)

    def need(group):
        if group not in waited:
            waited.add(group)
            semaphore_copy(
                arrived(group), 0, recv_index.setdefault(group, len(recv_index))
            ).wait_recv()

    def cell(plane, xx):
        return (plane * 2 + core) * NX + xx

    def block(plane, xx, yy, cols, first=0, rows=RB):
        start = pl.multiple_of(yy * RB + first, 16)
        return buf.at[cell(plane, xx), pl.ds(start, rows), pl.ds(*cols)]

    def y_group(plane, xx, cols, first=0, rows=NY * RB):
        return buf.at[cell(plane, xx), pl.ds(first, rows), pl.ds(*cols)]

    def x_group(plane, yy, cols, first=0, many=NX):
        start = pl.multiple_of(yy * RB, RB)
        return buf.at[
            pl.ds(cell(plane, 0) + first, many), pl.ds(start, RB), pl.ds(*cols)
        ]

    def plane_at(s):
        k = (s + 1) // 2
        return zm(-k if s % 2 else k)

    def x_cols(s):
        return X0_COLS if s == 0 else X_COLS

    def y_cols(s):
        return Y0_COLS if s == 0 else Y_COLS

    def lane_of(kind, s):
        return (kind, min(s, 1))

    both = (1, -1)

    def stage_a(s):
        if s:
            need(("Z", (s + 1) // 2))
        p = plane_at(s)
        for d in both if s else (1, -1, 2):
            send(("A", s), lane_of("A", s), block(p, x, y, x_cols(s)), at_y(d))
            send(("A", s), lane_of("A", s), block(p, x, y, y_cols(s)), at_x(d))

    def stage_b(s):
        need(("A", s))
        p = plane_at(s)
        half = RB // 2
        for d in both:
            first = 0 if d == 1 else half
            send(
                ("B", s),
                lane_of("B", s),
                block(p, x, ym(-d), x_cols(s), first, half),
                at_y(d),
            )
            send(
                ("B", s),
                lane_of("B", s),
                block(p, xm(-d), y, y_cols(s), first, half),
                at_x(d),
            )

    def stage_c(s):
        need(("B", s) if s else ("A", s))
        p = plane_at(s)
        for d in both:
            send(("C", s), lane_of("C", s), y_group(p, x, x_cols(s)), at_x(d))
            send(("C", s), lane_of("C", s), x_group(p, y, y_cols(s)), at_y(d))

    def over(s, ref):
        send(("S", s), ("S",), ref, sibling)

    def stage_d(s):
        need(("C", s))
        p = plane_at(s)
        for d in both:
            first = 0 if d == 1 else 2
            send(
                ("D", s),
                lane_of("D", s),
                y_group(p, xm(-d), x_cols(s), first * RB, 2 * RB),
                at_x(d),
            )
            send(
                ("D", s),
                lane_of("D", s),
                x_group(p, ym(-d), y_cols(s), first, 2),
                at_y(d),
            )
        for d in (0, 1, -1):
            over(s, y_group(p, xm(d), x_cols(s)))
            over(s, x_group(p, ym(d), y_cols(s)))

    def stage_e(s):
        need(("D", s))
        p = plane_at(s)
        over(s, y_group(p, xm(2), x_cols(s)))
        over(s, x_group(p, ym(2), y_cols(s)))

    def stage_w(h, g):
        if h == 1:
            need((("A", 0), ("C", 0), ("C", 0), ("D", 0))[g])
        else:
            need(("W", h - 1, g))
        for d in both:
            final = (g < 2) == (d == 1)
            piece = y_group(zm(-d * (h - 1)), xm(W_OFF[g]), W_COLS)
            if h < 4 or (h == 4 and final):
                send(("W", h, g), ("W",), piece, at_z(d))
            if h > 1 and (h < 5 or final):
                over(2 * (h - 1) - (1 if d == 1 or h == 5 else 0), piece)

    def stage_z(h):
        if h > 1:
            need(("Z", h - 1))
        for d in both:
            cols = ZB_COLS if h < 4 else (Y_COLS if d == 1 else X_COLS)
            send(("Z", h), ("Z",), block(zm(-d * (h - 1)), x, y, cols), at_z(d))
        if h > 1:
            need(("sc", h - 1))
        if h == 1:
            for d in (1, 2, 3):
                send(("sc", 1), ("sc", 1), sbuf.at[z, core, x * NY + y], at_y(d))
        elif h == 2:
            for d in (1, 2, 3):
                send(("sc", 2), ("sc", 2), sbuf.at[z, core, pl.ds(x * NY, NY)], at_x(d))
        elif h == 3:
            for d in range(1, NZ):
                send(("sc", 3), ("sc", 3), sbuf.at[z, core], at_z(d))
        else:
            send(("sc", 4), ("sc", 4), sbuf.at[:, core], sibling)

    stages = {
        "A": stage_a,
        "B": stage_b,
        "C": stage_c,
        "D": stage_d,
        "E": stage_e,
        "W": stage_w,
        "Z": stage_z,
    }

    def comm(point):
        for step in PLAN[point]:
            stages[step[0]](*step[1:])

    def drain():
        for lane, i in send_index.items():
            size = totals[lane]
            ref = scale_ref(size // 512) if lane[0] == "sc" else dummy(size // 8192)
            semaphore_copy(ref, i, 0).wait_send()

    def codes_of(plane, cc):
        return buf[pl.ds((plane * 2 + cc) * NX, NX)].reshape(NX * NY * RB, width)

    def scores(plane, cc, out):
        codes = codes_of(plane, cc)
        for first in range(0, q_ref.shape[0], ROWS):
            rows = pl.ds(first, ROWS)
            out[rows, :] = lax.dot_general(
                q_ref[rows, :],
                codes,
                (((1,), (1,)), ((), ())),
                preferred_element_type=jnp.float32,
            )

    def fold(values, op):
        out = values[:, 0:128]
        for j in range(1, values.shape[1] // 128):
            out = op(out, values[:, j * 128 : (j + 1) * 128])
        return out

    def consume(plane, cc, raw):
        codes = codes_of(plane, cc)
        count = codes.shape[0]
        by_y = sbuf[plane, cc]
        scales = jnp.concatenate(
            [jnp.sum(by_y[i * NY : (i + 1) * NY], axis=0) for i in range(NX)], axis=1
        )
        factor = scales * (temper * LOG2E)
        start = (plane * 2 + cc) * count
        for first in range(0, q_ref.shape[0], ROWS):
            rows = pl.ds(first, ROWS)
            s = raw[rows, :] * factor
            old = run_max[rows, :]
            new = jnp.maximum(
                old, jnp.max(fold(s, jnp.maximum), axis=1, keepdims=True)
            )
            run_max[rows, :] = new
            alpha = jnp.exp2(old - new)
            p = jnp.exp2(s - new[:, 0:1])
            hit = lax.broadcasted_iota(jnp.int32, s.shape, 1) == (
                pos[rows, 0:1] - start
            )
            run_sum[rows, :] = run_sum[rows, :] * alpha + fold(p, jnp.add)
            chosen[rows, :] += fold(jnp.where(hit, s, 0.0), jnp.add)
            weights = jnp.where(hit, 0.0, p * scales).astype(jnp.bfloat16)
            onehot = jnp.where(hit, scales, 0.0).astype(jnp.bfloat16)
            spread = jnp.concatenate([alpha] * (width // 128), axis=1)
            acc[rows, :] = acc[rows, :] * spread + jnp.dot(
                weights, codes, preferred_element_type=jnp.float32
            )
            picked[rows, :] += jnp.dot(
                onehot, codes, preferred_element_type=jnp.float32
            )

    def diagonal():
        shape = (128, 128)
        return lax.broadcasted_iota(jnp.int32, shape, 0) == lax.broadcasted_iota(
            jnp.int32, shape, 1
        )

    def prepare():
        j = p_ref[...]
        device = j // RB
        w = device // 4
        jz = lax.rem(device, 4) * 2 + w // 32
        flat = (
            (jz * 2 + lax.rem(w, 2)) * NX + lax.rem(w // 8, NX)
        ) * (NY * RB) + lax.rem(w // 2, NY) * RB + lax.rem(j, RB)
        flat = flat.astype(jnp.float32)
        for i in range(flat.shape[0]):
            column = jnp.sum(
                jnp.where(diagonal(), flat[i : i + 1, :], 0.0), axis=1, keepdims=True
            )
            pos[pl.ds(i * 128, 128), :] = jnp.broadcast_to(
                column, (128, 128)
            ).astype(jnp.int32)
        run_max[...] = jnp.full_like(run_max, -1e30)
        run_sum[...] = jnp.zeros_like(run_sum)
        chosen[...] = jnp.zeros_like(chosen)
        acc[...] = jnp.zeros_like(acc)
        picked[...] = jnp.zeros_like(picked)

    comm(0)
    prepare()
    comm(1)
    scores(plane_at(0), core, s_a)

    def tick(t, carry):
        k = (t + 1) // 2
        here = lax.rem(z + k * (1 - 2 * lax.rem(t, 2)) + NZ, NZ)
        t1 = jnp.minimum(t + 1, SLOTS - 1)
        k = (t1 + 1) // 2
        after = lax.rem(z + k * (1 - 2 * lax.rem(t1, 2)) + NZ, NZ)
        for i in range(SLOTS):

            @pl.when(t == i)
            def _():
                comm(2 * i + 2)
                if i == 0:
                    need(("sc", 4))
                need(("S", i))

        scores(here, 1 - core, s_b)
        consume(here, core, s_a)
        for i in range(SLOTS - 1):
            if PLAN[2 * i + 3]:

                @pl.when(t == i)
                def _():
                    comm(2 * i + 3)

        scores(after, core, s_a)
        consume(here, 1 - core, s_b)
        return carry

    lax.fori_loop(0, SLOTS, tick, 0)
    drain()
    assert (len(send_index), len(recv_index)) == (N_SEND, N_RECV)

    total = jnp.sum(run_sum[...], axis=1, keepdims=True)
    lse = run_max[:, 0:1] + jnp.log2(total)
    score = jnp.sum(chosen[...], axis=1, keepdims=True)
    losses = (lse - score) * (1.0 / LOG2E)
    for i in range(loss_ref.shape[0]):
        loss_ref[pl.ds(i, 1), :] = jnp.sum(
            jnp.where(diagonal(), losses[i * 128 : (i + 1) * 128], 0.0),
            axis=0,
            keepdims=True,
        )
    extra = jnp.exp2(score - lse) - 1.0
    inverse = 1.0 / total
    grad_ref[...] = (temper * (acc[...] * inverse + extra * picked[...])).astype(
        grad_ref.dtype
    )


N_SEND = 14
N_RECV = 63


def shards(queries, documents, positives):
    count, width = queries.shape
    vmem = pl.BlockSpec(memory_space=pltpu.VMEM)
    f32 = jnp.float32
    losses, grad = pl.pallas_call(
        kernel,
        out_shape=(
            pltpu.VMEM((count // 128, 128), f32),
            pltpu.VMEM((count, width), queries.dtype),
        ),
        in_specs=[vmem] * 3,
        out_specs=(vmem, vmem),
        scratch_shapes=[
            pltpu.VMEM((NZ * 2 * NX, NY * RB, width), jnp.bfloat16),
            pltpu.VMEM((NZ, 2, NX * NY, 1, 128), f32),
            pltpu.VMEM((count, 128), jnp.int32),
            pltpu.VMEM((count, 128), f32),
            pltpu.VMEM((count, 128), f32),
            pltpu.VMEM((count, 128), f32),
            pltpu.VMEM((count, width), f32),
            pltpu.VMEM((count, width), f32),
            pltpu.VMEM((count, 512), f32),
            pltpu.VMEM((count, 512), f32),
            pltpu.SemaphoreType.DMA((N_SEND,)),
            pltpu.SemaphoreType.DMA((N_RECV,)),
        ],
        compiler_params=pltpu.CompilerParams(
            collective_id=0, has_side_effects=True, vmem_limit_bytes=56 * 2**20
        ),
        name="gather_softmax",
    )(queries, documents, positives.reshape(count // 128, 128))
    return losses.reshape(count), grad


def solution(mesh):
    placed = (P(("wide", "narrow"), None), P(("wide", "narrow"), None), P(("wide", "narrow")))
    return jax.shard_map(
        shards,
        mesh=mesh,
        in_specs=placed,
        out_specs=(P(("wide", "narrow")), P(("wide", "narrow"), None)),
        check_vma=False,
    )
```

```python
import jax
import jax.numpy as jnp
import numpy as np
from jax import lax
from jax.experimental import pallas as pl
from jax.experimental.pallas import tpu as pltpu
from jax.sharding import PartitionSpec as P

LOG2E = 1.4426950408889634
MESH = pl.DeviceIdType.MESH
NX, NY, NZ = 4, 4, 8
RB = 32
CHIPS = NX * NY * NZ
PER = 8
CHUNKS = CHIPS // PER
ROWS = 256
UNITS = RB * 768 * 2 // 512 + 1
LANE_BLOCKS = 10

OFFSETS = (
    (0, 0, 0), (1, 0, 0), (3, 0, 0), (0, 1, 0), (0, 3, 0), (0, 0, 1), (0, 0, 7), (2, 0, 0),
    (0, 2, 0), (0, 0, 6), (1, 1, 0), (3, 1, 0), (0, 1, 1), (1, 3, 0), (1, 0, 7), (1, 0, 1),
    (3, 3, 0), (0, 1, 7), (0, 3, 1), (0, 0, 2), (3, 0, 7), (3, 0, 1), (0, 3, 7), (0, 0, 4),
    (1, 2, 0), (3, 2, 0), (2, 1, 0), (2, 0, 1), (2, 0, 7), (2, 3, 0), (0, 2, 1), (0, 2, 7),
    (0, 1, 6), (1, 0, 6), (3, 0, 6), (0, 3, 6), (0, 1, 2), (1, 1, 1), (0, 0, 5), (3, 1, 1),
    (1, 3, 1), (1, 1, 7), (0, 3, 2), (1, 3, 7), (1, 0, 2), (3, 0, 2), (0, 0, 3), (0, 1, 4),
    (1, 0, 4), (3, 3, 7), (3, 1, 7), (3, 3, 1), (2, 0, 2), (1, 2, 1), (2, 1, 1), (0, 1, 5),
    (3, 2, 1), (2, 3, 1), (0, 2, 2), (1, 2, 7), (2, 1, 7), (1, 0, 5), (3, 2, 7), (2, 3, 7),
    (0, 1, 3), (1, 1, 6), (3, 1, 6), (3, 0, 5), (3, 3, 6), (1, 3, 6), (1, 1, 2), (2, 0, 6),
    (0, 2, 6), (0, 3, 5), (3, 1, 2), (2, 2, 0), (0, 3, 3), (1, 3, 2), (0, 2, 4), (1, 0, 3),
    (3, 0, 3), (3, 3, 2), (2, 0, 4), (1, 1, 4), (2, 0, 3), (1, 2, 6), (3, 0, 4), (0, 3, 4),
    (2, 0, 5), (0, 2, 5), (0, 2, 3), (2, 1, 6), (3, 1, 5), (1, 3, 5), (1, 2, 2), (1, 1, 3),
    (2, 1, 2), (3, 3, 5), (3, 1, 3), (2, 3, 2), (3, 2, 2), (1, 1, 5), (3, 2, 6), (2, 3, 6),
    (2, 2, 1), (2, 2, 7), (1, 3, 3), (1, 2, 4), (3, 3, 3), (1, 3, 4), (2, 1, 3), (1, 2, 5),
    (2, 2, 6), (3, 2, 5), (2, 3, 3), (2, 1, 5), (2, 1, 4), (3, 1, 4), (2, 3, 5), (1, 2, 3),
    (3, 3, 4), (3, 2, 3), (2, 2, 2), (3, 2, 4), (2, 3, 4), (2, 2, 4), (2, 2, 3), (2, 2, 5),
)

GROUPS = (6, 1, 1, 1, 5, 6, 3, 4, 2, 2, 4, 4, 2, 4, 1, 2, 1, 2, 6, 6, 6, 6, 6, 2, 6, 4, 6, 6, 4, 5, 4, 6, 1, 2)

PLAN = (
    ((0, 0, 0, 1, 0), (0, 1, 0, 2, 0), (0, 2, 0, 3, 0), (0, 3, 0, 4, 0), (0, 4, 0, 5, 0), (0, 5, 0, 6, 0), (0, 6, 0, 23, 1), (0, 7, 0, 7, 2), (0, 8, 0, 8, 3), (2, 0, 1),),
    ((1, 0), (0, 5, 6, 9, 4), (0, 0, 3, 10, 4), (0, 1, 3, 11, 4), (0, 2, 5, 12, 4), (0, 3, 1, 13, 4), (2, 1, 7), (0, 5, 1, 14, 5), (0, 0, 5, 15, 5), (0, 1, 4, 16, 5), (0, 2, 6, 17, 5), (0, 3, 5, 18, 5), (0, 4, 5, 19, 5), (0, 5, 2, 20, 6), (0, 1, 5, 21, 6), (0, 3, 6, 22, 6), (1, 2), (0, 2, 7, 26, 7), (0, 4, 7, 27, 7), (0, 5, 7, 28, 7), (0, 3, 7, 29, 7), (2, 7, 8), (1, 3), (0, 0, 8, 24, 8), (0, 1, 8, 25, 8), (2, 8, 9), (0, 4, 8, 30, 9), (0, 5, 8, 31, 9), (1, 4), (0, 2, 9, 32, 10), (0, 0, 9, 33, 10), (0, 1, 9, 34, 10), (0, 3, 9, 35, 10), (2, 9, 14),),
    ((0, 4, 12, 36, 11), (0, 0, 12, 37, 11), (0, 5, 9, 38, 11), (0, 1, 12, 39, 11), (0, 4, 13, 40, 12), (0, 5, 10, 41, 12), (1, 5), (0, 3, 14, 43, 13), (0, 0, 19, 44, 13), (0, 1, 19, 45, 13), (0, 3, 19, 42, 14), (0, 4, 19, 46, 13), (2, 14, 16), (2, 16, 20), (0, 5, 16, 49, 15), (0, 1, 17, 50, 15), (1, 6), (0, 3, 21, 51, 16), (2, 20, 23), (1, 1), (0, 2, 23, 47, 17), (0, 0, 23, 48, 17), (2, 23, 24),),
    ((1, 8), (1, 7), (1, 9), (1, 10), (0, 4, 27, 52, 18), (0, 0, 30, 53, 18), (0, 2, 27, 54, 18), (0, 5, 32, 55, 18), (0, 1, 30, 56, 18), (0, 3, 27, 57, 18), (0, 4, 30, 58, 19), (0, 0, 31, 59, 19), (0, 2, 28, 60, 19), (0, 5, 33, 61, 19), (0, 1, 31, 62, 19), (0, 3, 28, 63, 19), (2, 24, 32), (2, 32, 36),),
    ((1, 11), (0, 4, 36, 64, 20), (0, 0, 32, 65, 20), (0, 2, 34, 66, 20), (0, 5, 34, 67, 20), (0, 1, 35, 68, 20), (0, 3, 33, 69, 20), (0, 4, 37, 70, 21), (0, 0, 33, 71, 21), (0, 2, 32, 72, 21), (0, 5, 35, 73, 21), (0, 1, 36, 74, 21), (0, 3, 29, 75, 21), (2, 36, 40), (1, 12), (2, 40, 42), (1, 14), (2, 42, 43),),
    ((1, 13), (1, 17), (1, 15), (1, 16), (0, 4, 42, 76, 22), (0, 0, 42, 77, 22), (0, 2, 47, 78, 22), (0, 5, 48, 79, 22), (0, 1, 46, 80, 22), (0, 3, 45, 81, 22), (0, 0, 48, 82, 23), (0, 2, 48, 83, 23), (2, 43, 48), (2, 48, 52),),
    ((1, 18), (1, 19), (0, 4, 52, 84, 24), (0, 5, 59, 85, 24), (0, 1, 23, 86, 24), (0, 3, 23, 87, 24), (0, 4, 58, 90, 25), (0, 0, 61, 88, 24), (0, 2, 55, 89, 24), (0, 5, 60, 91, 25), (0, 1, 55, 92, 25), (0, 3, 61, 93, 25), (2, 52, 56), (2, 56, 64),),
    ((1, 20), (0, 4, 53, 94, 26), (0, 0, 64, 95, 26), (0, 2, 52, 96, 26), (0, 5, 68, 97, 26), (0, 1, 64, 98, 26), (0, 3, 52, 99, 26), (0, 4, 56, 100, 27), (0, 0, 55, 101, 27), (0, 2, 66, 102, 27), (0, 5, 63, 103, 27), (0, 1, 56, 104, 27), (0, 3, 63, 105, 27), (2, 64, 70),),
    ((1, 21), (1, 22), (0, 4, 77, 106, 28), (0, 0, 78, 107, 28), (0, 1, 76, 108, 28), (0, 3, 48, 109, 28), (2, 70, 72), (2, 72, 80), (2, 80, 82),),
    ((1, 23), (1, 24), (0, 2, 84, 110, 29), (0, 5, 85, 111, 29), (0, 0, 85, 112, 29), (0, 1, 89, 113, 29), (0, 3, 84, 114, 29), (0, 2, 88, 115, 30), (0, 0, 83, 116, 30), (0, 1, 47, 117, 30), (0, 3, 88, 118, 30), (2, 82, 88), (2, 88, 90), (1, 25), (2, 90, 94),),
    ((1, 26), (0, 4, 94, 119, 31), (0, 5, 97, 120, 31), (0, 2, 98, 121, 31), (0, 0, 94, 122, 31), (0, 1, 78, 123, 31), (0, 3, 82, 124, 31), (2, 94, 96), (2, 96, 100),),
    ((1, 27), (1, 28), (0, 0, 107, 125, 32), (2, 100, 104), (2, 104, 110),),
    ((1, 29), (0, 2, 110, 126, 33), (0, 0, 111, 127, 33), (2, 110, 112), (2, 112, 115),),
    ((1, 30), (1, 31), (2, 115, 120), (2, 120, 125),),
    ((1, 32), (2, 125, 126),),
    ((1, 33), (2, 126, 128),),
    (),
    (),
)


N_SENT = sum(step[0] == 0 for point in PLAN for step in point)
N_LANES = -(-N_SENT // LANE_BLOCKS)


def offset_table():
    table = np.zeros((CHUNKS, PER * RB * 2), np.int32)
    for k in range(CHUNKS):
        for side in range(2):
            for b in range(PER):
                ox, oy, oz = OFFSETS[k * PER + b]
                first = (side * PER + b) * RB
                table[k, first : first + RB] = (
                    ox + oy * 4 + oz * 16 + side * 128 + np.arange(RB) * 256
                )
    return table


def kernel(
    q_hbm,
    d_ref,
    p_ref,
    table_ref,
    loss_ref,
    grad_ref,
    buf,
    sbuf,
    pos,
    ids,
    run_max,
    run_sum,
    chosen,
    acc,
    picked,
    s_a,
    s_b,
    q_ref,
    send_sem,
    recv_sem,
    load_sem,
):
    wide = lax.axis_index("wide")
    narrow = lax.axis_index("narrow")
    core = lax.rem(wide, 2)
    y = lax.rem(wide // 2, NY)
    x = lax.rem(wide // 8, NX)
    z = narrow * 2 + wide // 32
    width = q_ref.shape[1]
    temper = width**-0.5

    def dev(dx, dy, dz, cc):
        xx = lax.rem(x + dx + NX, NX)
        yy = lax.rem(y + dy + NY, NY)
        zz = lax.rem(z + dz + NZ, NZ)
        return ((lax.rem(zz, 2) * NX + xx) * NY + yy) * 2 + cc, zz // 2

    sibling = dev(0, 0, 0, 1 - core)
    peers = [
        dev(*d, core)
        for d in (
            (1, 0, 0),
            (-1, 0, 0),
            (0, 1, 0),
            (0, -1, 0),
            (0, 0, 1),
            (0, 0, -1),
            (0, 0, 4),
            (2, 0, 0),
            (0, 2, 0),
        )
    ]

    barrier = pltpu.get_barrier_semaphore()
    for peer in peers + [sibling]:
        pl.semaphore_signal(barrier, inc=1, device_id=peer, device_id_type=MESH)
    load = pltpu.make_async_copy(q_hbm, q_ref, load_sem)
    load.start()

    docs = d_ref[...].astype(jnp.float32)
    scale = jnp.max(jnp.abs(docs), axis=1, keepdims=True) + 1e-06
    buf[0, 0] = (docs / scale).astype(jnp.bfloat16)
    lane = lax.broadcasted_iota(jnp.int32, (RB, 128), 1)
    row = lax.broadcasted_iota(jnp.int32, (RB, 128), 0)
    sbuf[0] = jnp.sum(
        jnp.where((lane & (RB - 1)) == row, scale, 0.0), axis=0, keepdims=True
    )
    pl.semaphore_wait(barrier, len(peers) + 1)

    lanes = [0] * N_LANES
    count = [0]

    def remote(src, dst, send_at, recv_at, peer):
        return pltpu.make_async_remote_copy(
            src_ref=src,
            dst_ref=dst,
            send_sem=send_sem.at[send_at],
            recv_sem=recv_sem.at[recv_at],
            device_id=peer,
            device_id_type=MESH,
        )

    def whole(blocks):
        return sbuf.at[pl.ds(0, blocks * UNITS)]

    def send(direction, here, there, group):
        at = count[0] // LANE_BLOCKS
        count[0] += 1
        lanes[at] += 1
        peer = peers[direction]
        remote(buf.at[0, here], buf.at[0, there], at, group, peer).start()
        remote(sbuf.at[here], sbuf.at[there], at, group, peer).start()

    def arrive(group):
        ref = whole(GROUPS[group])
        remote(ref, ref, 0, group, sibling).wait_recv()

    def over(first, end):
        k, many = first // PER, end - first
        here, there = pl.ds(first, many), pl.ds(CHIPS + first, many)
        at, group = N_LANES + k, len(GROUPS) + k
        remote(buf.at[0, here], buf.at[1, here], at, group, sibling).start()
        remote(sbuf.at[here], sbuf.at[there], at, group, sibling).start()

    def comm(point):
        for step in PLAN[point]:
            (send, arrive, over)[step[0]](*step[1:])

    def chunk_here(k):
        ref = whole(PER)
        remote(ref, ref, 0, len(GROUPS) + k, sibling).wait_recv()

    def drain():
        for i, blocks in enumerate(lanes + [PER] * CHUNKS):
            ref = whole(blocks)
            remote(ref, ref, i, 0, sibling).wait_send()

    def codes_of(k):
        part = pl.ds(k * PER, PER)
        return jnp.concatenate(
            [buf[side, part].reshape(PER * RB, width) for side in range(2)], axis=0
        )

    def scores(k, out):
        codes = codes_of(k)
        for first in range(0, q_ref.shape[0], ROWS):
            rows = pl.ds(first, ROWS)
            out[rows, :] = lax.dot_general(
                q_ref[rows, :],
                codes,
                (((1,), (1,)), ((), ())),
                preferred_element_type=jnp.float32,
            )

    def fold(values, op):
        out = values[:, 0:128]
        for j in range(1, values.shape[1] // 128):
            out = op(out, values[:, j * 128 : (j + 1) * 128])
        return out

    def scales_of(k):
        quarter = lax.broadcasted_iota(jnp.int32, (1, 128), 1) // RB
        parts = []
        for side in range(2):
            for half in range(2):
                four = sbuf[pl.ds(side * CHIPS + k * PER + half * 4, 4)]
                part = four[0]
                for b in range(1, 4):
                    part = jnp.where(quarter == b, four[b], part)
                parts.append(part)
        return jnp.concatenate(parts, axis=1)

    def consume(k, raw):
        codes = codes_of(k)
        scales = scales_of(k)
        names = ids[pl.ds(k, 1), :]
        factor = scales * (temper * LOG2E)
        for first in range(0, q_ref.shape[0], ROWS):
            rows = pl.ds(first, ROWS)
            s = raw[rows, :] * factor
            old = run_max[rows, :]
            new = jnp.maximum(
                old, jnp.max(fold(s, jnp.maximum), axis=1, keepdims=True)
            )
            run_max[rows, :] = new
            alpha = jnp.exp2(old - new)
            p = jnp.exp2(s - new[:, 0:1])
            hit = names == pos[rows, 0:1]
            run_sum[rows, :] = run_sum[rows, :] * alpha + fold(p, jnp.add)
            chosen[rows, :] += fold(jnp.where(hit, s, 0.0), jnp.add)
            weights = jnp.where(hit, 0.0, p * scales).astype(jnp.bfloat16)
            onehot = jnp.where(hit, scales, 0.0).astype(jnp.bfloat16)
            spread = jnp.concatenate([alpha] * (width // 128), axis=1)
            acc[rows, :] = acc[rows, :] * spread + jnp.dot(
                weights, codes, preferred_element_type=jnp.float32
            )
            picked[rows, :] += jnp.dot(
                onehot, codes, preferred_element_type=jnp.float32
            )

    def diagonal():
        shape = (128, 128)
        return lax.broadcasted_iota(jnp.int32, shape, 0) == lax.broadcasted_iota(
            jnp.int32, shape, 1
        )

    def prepare():
        wanted = p_ref[...].astype(jnp.float32)
        for i in range(wanted.shape[0]):
            column = jnp.sum(
                jnp.where(diagonal(), wanted[i : i + 1, :], 0.0), axis=1, keepdims=True
            )
            pos[pl.ds(i * 128, 128), :] = jnp.broadcast_to(
                column, (128, 128)
            ).astype(jnp.int32)
        table = table_ref[...]
        sx = (x - (table & 3)) & 3
        sy = (y - ((table >> 2) & 3)) & 3
        sz = (z - ((table >> 4) & 7)) & 7
        sc = (core + ((table >> 7) & 1)) & 1
        device = ((((sz & 1) * NX + sx) * NY + sy) * 2 + sc) * 4 + (sz >> 1)
        ids[...] = device * RB + (table >> 8)
        run_max[...] = jnp.full_like(run_max, -1e30)
        run_sum[...] = jnp.zeros_like(run_sum)
        chosen[...] = jnp.zeros_like(chosen)
        acc[...] = jnp.zeros_like(acc)
        picked[...] = jnp.zeros_like(picked)

    comm(0)
    prepare()
    comm(1)
    load.wait()
    chunk_here(0)
    scores(0, s_a)

    def pair(t, carry):
        for i in range(CHUNKS // 2):

            @pl.when(t == i)
            def _():
                comm(2 * i + 2)
                chunk_here(2 * i + 1)

        scores(2 * t + 1, s_b)
        consume(2 * t, s_a)
        for i in range(CHUNKS // 2 - 1):

            @pl.when(t == i)
            def _():
                comm(2 * i + 3)
                chunk_here(2 * i + 2)

        scores(jnp.minimum(2 * t + 2, CHUNKS - 1), s_a)
        consume(2 * t + 1, s_b)
        return carry

    lax.fori_loop(0, CHUNKS // 2, pair, 0)
    drain()

    total = jnp.sum(run_sum[...], axis=1, keepdims=True)
    lse = run_max[:, 0:1] + jnp.log2(total)
    score = jnp.sum(chosen[...], axis=1, keepdims=True)
    losses = (lse - score) * (1.0 / LOG2E)
    for i in range(loss_ref.shape[0]):
        loss_ref[pl.ds(i, 1), :] = jnp.sum(
            jnp.where(diagonal(), losses[i * 128 : (i + 1) * 128], 0.0),
            axis=0,
            keepdims=True,
        )
    extra = jnp.exp2(score - lse) - 1.0
    inverse = 1.0 / total
    grad_ref[...] = (temper * (acc[...] * inverse + extra * picked[...])).astype(
        grad_ref.dtype
    )


def shards(queries, documents, positives):
    count, width = queries.shape
    vmem = pl.BlockSpec(memory_space=pltpu.VMEM)
    f32 = jnp.float32
    losses, grad = pl.pallas_call(
        kernel,
        out_shape=(
            pltpu.VMEM((count // 128, 128), f32),
            pltpu.VMEM((count, width), queries.dtype),
        ),
        in_specs=[pl.BlockSpec(memory_space=pltpu.HBM), vmem, vmem, vmem],
        out_specs=(vmem, vmem),
        scratch_shapes=[
            pltpu.VMEM((2, CHIPS, RB, width), jnp.bfloat16),
            pltpu.VMEM((LANE_BLOCKS * UNITS, 1, 128), f32),
            pltpu.VMEM((count, 128), jnp.int32),
            pltpu.VMEM((CHUNKS, PER * RB * 2), jnp.int32),
            pltpu.VMEM((count, 128), f32),
            pltpu.VMEM((count, 128), f32),
            pltpu.VMEM((count, 128), f32),
            pltpu.VMEM((count, width), f32),
            pltpu.VMEM((count, width), f32),
            pltpu.VMEM((count, PER * RB * 2), f32),
            pltpu.VMEM((count, PER * RB * 2), f32),
            pltpu.VMEM((count, width), queries.dtype),
            pltpu.SemaphoreType.DMA((N_LANES + CHUNKS,)),
            pltpu.SemaphoreType.DMA((len(GROUPS) + CHUNKS,)),
            pltpu.SemaphoreType.DMA,
        ],
        compiler_params=pltpu.CompilerParams(
            collective_id=0, has_side_effects=True, vmem_limit_bytes=56 * 2**20
        ),
        name="gather_softmax",
    )(
        queries,
        documents,
        positives.reshape(count // 128, 128),
        jnp.asarray(offset_table()),
    )
    return losses.reshape(count), grad


def solution(mesh):
    placed = (P(("wide", "narrow"), None), P(("wide", "narrow"), None), P(("wide", "narrow")))
    return jax.shard_map(
        shards,
        mesh=mesh,
        in_specs=placed,
        out_specs=(P(("wide", "narrow")), P(("wide", "narrow"), None)),
        check_vma=False,
    )
```
